32 devices in a mesh: base: 4 (over y, x), slab: 8 (over z, core).
Axes of the slice: x: 2, y: 2, z: 4, core: 2. Of those that a mesh axis runs over, the one named last changes fastest.
Arguments:
- residual: float32 [4096, 2, 128], P(('base', 'slab')), may hold values from -6 to 6
- position: float32 [4096, 2, 128], P(('base', 'slab')), may hold values from 4 to 124
- owner: int32 [4096, 1], P(('base', 'slab')), may hold values from 0 to 31; in each aligned block of 128 rows (0 to 127, 128 to 255, ...) at most 8 rows name the same one
- tile_local: int32 [4096], P(('base', 'slab')), may hold values from 0 to 127
- xi: float32 [4096, 4096], P(('base', 'slab')), may hold values from -6 to 6
- amplitude: float32 [4096, 4096], P(('base', 'slab')), may hold values from 0.05 to 0.5
Outputs:
- gradient: float32 [4096, 4096], P(('base', 'slab'))
The draws below stay inside these ranges and needn't reach their ends.
Inputs may be any that keep to these rules, and one draw needn't show every extreme that they name: Among the blocks of one device no owner region is named by more than 8 blocks, a bound that some owner region reaches on some device.
All inputs are finite; a program needn't handle non-finite values.
Results may differ from the reference program's by a relative error of at most 0.00065.
Values sent between devices are 32-bit elements; how exact they have to be, the bound alone decides.
A program may use at most 128 MiB of HBM per device.

```python
import math
import jax
import jax.numpy as jnp
import numpy as np
from jax import lax

G = 8192
IMG = 4096
TILE = 128
VB = 128
BLK_DEV = 128
BLOCKS = 4096
CAP = 8
TILES_REG = 128
N_BASE = 4
N_SLAB = 8
DEVICES = 32


def with_ends(values, own_key, low, top_value):
    longest = values.shape.index(max(values.shape))
    spots = []
    for shift in (0, 1):
        where = [jax.random.randint(jax.random.fold_in(own_key, axis), (), 0, length) for axis, length in enumerate(values.shape)]
        where[longest] = (where[longest] + shift) % values.shape[longest]
        spots.append(tuple(where))
    return values.at[spots[0]].set(low).at[spots[1]].set(top_value)


def block_scale(key, dims, split, least, top_value):
    def one(axis_at, blocks):
        heights = jax.random.uniform(jax.random.fold_in(jax.random.fold_in(key, 6), axis_at), (blocks,), jnp.float32, least / len(split), top_value / len(split))
        return jnp.repeat(jnp.exp(heights), dims[axis_at] // blocks).reshape((-1,) + (1,) * (len(dims) - axis_at - 1))

    gain = one(*split[0])
    for cut in split[1:]:
        gain = gain * one(*cut)
    return gain


def deal_out(key, own, number, rows, count, top, reach, skew):
    ranking = jax.random.permutation(key, count)
    packed, usual = portions_of(count, rows * top, reach, skew, True), portions_of(count, rows * top, reach, skew, False)
    places = jnp.arange(count)

    def named(tallies, rotation):
        used = int((tallies > 0).sum())
        fixed = max(1, used // 4)
        moved = fixed + (places - fixed + rotation * (used - fixed)) % max(1, count - fixed)
        return jnp.zeros((count,), jnp.int32).at[ranking[jnp.where(places < fixed, places, moved)]].set(jnp.asarray(tallies, jnp.int32))

    tallies = jnp.where(number % 4 == 0, named(packed, number // 4), named(usual, number - number // 4 - 1))
    mixed = jax.random.permutation(jax.random.fold_in(own, 3), count)
    donor, sink = mixed[0:count // 2 * 2:2], mixed[1:count // 2 * 2:2]
    room = jnp.minimum(tallies[donor] - 1, reach - tallies[sink]) // 2
    room = jnp.where((donor == ranking[0]) | (sink == ranking[0]) | (tallies[sink] == 0), 0, jnp.maximum(room, 0))
    moved = jax.random.randint(jax.random.fold_in(own, 4), (count // 2,), 0, 1 << 20) % (room + 1)
    tallies = tallies.at[donor].add(-moved).at[sink].add(moved)
    members = jnp.searchsorted(jnp.cumsum(tallies), jnp.arange(rows * top), side="right").astype(jnp.int32)
    table = members.reshape(top, rows).T
    table = table[jax.random.permutation(jax.random.fold_in(own, 1), rows)]
    rotation = jax.random.randint(jax.random.fold_in(own, 2), (rows, 1), 0, top)
    return jnp.take_along_axis(table, (jnp.arange(top)[None, :] + rotation) % top, axis=1)


def portions_of(amount, total, limit, slope, full):
    weights = [(1 << 20) // math.isqrt(standing ** slope) + 1 for standing in range(1, amount + 1)]
    largest = limit if full else min(limit, max(-(-total // amount), total * weights[0] // sum(weights)))
    least = 1 if total - largest >= amount - 1 else 0
    holding, rest = [largest] + [least] * (amount - 1), total - largest - least * (amount - 1)
    while rest > 0:
        movable = [i for i in range(1, amount) if holding[i] < largest] or [i for i in range(1, amount) if holding[i] < limit]
        whole, remaining = sum([weights[i] for i in movable]), rest
        for i in movable:
            addition = min(limit - holding[i], max(1, remaining * weights[i] // whole), rest)
            holding[i] = holding[i] + addition
            rest = rest - addition
    return np.array(holding)


def gaussian(rng, shape, width, limit, split=(), kind=jnp.bfloat16):
    result = width * jax.random.normal(rng, shape, jnp.float32)
    if split:
        result = result * block_scale(rng, shape, split, -0.22, 0.18)
    return jnp.clip(result, -limit, limit).astype(kind)


def setup_inputs(seed: int = 0) -> dict:
    keys = jax.random.split(jax.random.key(seed), 7)
    residual = gaussian(keys[0], (BLOCKS, 2, VB), 1.0, 6.0, ((0, 32),), jnp.float32)
    position = jnp.clip(4.0 + 120.0 * jax.random.uniform(keys[1], (BLOCKS, 2, VB), jnp.float32) ** block_scale(keys[1], (BLOCKS, 2, VB), ((0, 32),), -0.2, 0.2), 4.0, 124.0)
    owner_keys = jax.random.split(jax.random.fold_in(keys[2], 1), BLOCKS // BLK_DEV)
    owner_turns = jax.random.permutation(jax.random.fold_in(keys[2], 3), BLOCKS // BLK_DEV)
    owner = jax.vmap(lambda own, number: deal_out(jax.random.fold_in(keys[2], 2), own, number, BLK_DEV, DEVICES, 1, CAP, 2))(owner_keys, owner_turns).reshape((BLOCKS, 1))
    tile_local = with_ends(jax.random.randint(keys[3], (BLOCKS,), 0, TILES_REG), jax.random.fold_in(keys[3], 1), 0, TILES_REG - 1).astype(jnp.int32)
    xi = gaussian(keys[4], (IMG, IMG), 1.0, 6.0, ((0, 32),), jnp.float32)
    amplitude = jnp.clip(jnp.exp(math.log(0.5) - 2.3025851 * jax.random.uniform(keys[5], (IMG, IMG), jnp.float32) ** block_scale(keys[5], (IMG, IMG), ((0, 32),), -0.2, 0.2)), 0.05, 0.5)
    return dict(residual=residual, position=position, owner=owner, tile_local=tile_local, xi=xi, amplitude=amplitude)


def taps(offsets):
    cells = jnp.arange(TILE, dtype=jnp.float32)
    scaled = (cells[None, :, None] - offsets[:, None, :]) * 0.25
    return jnp.maximum(1.0 - scaled * scaled, 0.0) ** 3


def reference(residual, position, owner, tile_local, xi, amplitude):
    rows_tiles = G // N_SLAB // TILE
    cols_tiles = G // N_BASE // TILE
    across = G // TILE
    target = owner[:, 0]
    tile_row = ((target % N_SLAB) * rows_tiles + tile_local // cols_tiles).astype(jnp.int32)
    tile_col = ((target // N_SLAB) * cols_tiles + tile_local % cols_tiles).astype(jnp.int32)

    def step(total, index):
        start = (index * BLK_DEV).astype(jnp.int32)
        values = lax.dynamic_slice_in_dim(residual, start, BLK_DEV, 0)
        places = lax.dynamic_slice_in_dim(position, start, BLK_DEV, 0)
        rows = lax.dynamic_slice_in_dim(tile_row, start, BLK_DEV, 0)
        cols = lax.dynamic_slice_in_dim(tile_col, start, BLK_DEV, 0)
        row_taps = taps(places[:, 0, :])
        col_taps = taps(places[:, 1, :])
        weighted = jnp.concatenate([col_taps * values[:, 0:1, :], col_taps * values[:, 1:2, :]], axis=1)
        subgrid = jnp.einsum("grv,gkv->grk", row_taps, weighted, precision=lax.Precision.HIGHEST)
        total = total.at[rows, cols].add(subgrid.reshape(BLK_DEV, TILE, 2, TILE))
        return total, None

    empty = jnp.zeros((across, across, TILE, 2, TILE), jnp.float32)
    tiles = lax.scan(step, empty, jnp.arange(DEVICES, dtype=jnp.int32))[0]
    grid = tiles.transpose(3, 0, 2, 1, 4).reshape(2, G, G)
    wave = jnp.fft.ifft2(grid[0] + 1j * grid[1])
    lower = G // 4
    back = jnp.real(wave[lower:lower + IMG, lower:lower + IMG]) * G
    spectrum = jnp.fft.fft2(amplitude * xi)
    sky = jnp.exp((jnp.real(spectrum) - jnp.imag(spectrum)) / IMG)
    folded = jnp.fft.fft2(sky * back)
    return amplitude * (jnp.real(folded) - jnp.imag(folded)) / IMG
```

```python
import functools

import jax
import jax.numpy as jnp
import numpy as np
from jax import lax
from jax.experimental import pallas as pl
from jax.experimental.pallas import tpu as pltpu
from jax.sharding import PartitionSpec as P

G = 8192
TILE = 128
both = ("base", "slab")
fine = lax.Precision.HIGHEST


def trig(product, modulus):
    angle = (product % modulus).astype(np.float64) * (2.0 * np.pi / modulus)
    return np.cos(angle), np.sin(angle)


def column_table(n, size):
    depth = size // n
    half = depth // 2
    i = np.arange(half)[None, :]
    j = np.arange(n)[:, None]
    low = n * i + j
    high = (-low) % size
    high[0, 0] = size // 2
    return np.concatenate([low, high], axis=1)


def row_tables(n, size):
    depth = size // n
    cols = column_table(n, size)
    oc, osn = trig(np.arange(n)[:, None] * np.arange(n)[None, :], n)
    outer = np.stack([oc, osn], axis=1)
    prod = np.arange(depth)[None, :, None] * cols[:, None, :]
    c, s = trig(prod, size)
    sign = np.where(np.arange(depth) < depth // 2, 1.0, -1.0)[None, None, :]
    inner = np.stack([c + s, sign * (c - s)], axis=1)
    return outer.astype(np.float32), inner.astype(np.float32)


def grid_row_tables(n, size):
    depth = G // n
    cols = column_table(n, size)
    half = cols.shape[1] // 2
    oc, osn = trig(np.arange(n)[:, None] * np.arange(n)[None, :], n)
    outer = np.stack([np.stack([oc, osn], 1), np.stack([-osn, oc], 1)], 0)
    low = cols[:, :half]
    high = cols[(-np.arange(n)) % n, half:]
    a = np.arange(depth)[None, :, None]
    out = []
    for part in (low, high):
        c, s = trig(a * (part[:, None, :] + G // 4), G)
        out.append(np.stack([np.concatenate([c, s], 2), np.concatenate([-s, c], 2)], 1))
    return outer.astype(np.float32), out[0].astype(np.float32), out[1].astype(np.float32)


def taps(cells, offsets):
    scaled = (cells - offsets) * 0.25
    kept = jnp.maximum(1.0 - scaled * scaled, 0.0)
    return kept * kept * kept


def split_three(x):
    high = x.astype(jnp.bfloat16)
    rest = x - high.astype(jnp.float32)
    middle = rest.astype(jnp.bfloat16)
    return high, middle, (rest - middle.astype(jnp.float32)).astype(jnp.bfloat16)


def grid_kernel(rows, info_ref, list_ref, res_ref, pos_ref, out_ref):
    count = info_ref[0]
    first = info_ref[1].astype(jnp.float32)
    out_ref[...] = jnp.zeros_like(out_ref)
    row_cells = lax.broadcasted_iota(jnp.int32, (rows, TILE), 0).astype(jnp.float32) + first
    col_cells = lax.broadcasted_iota(jnp.int32, (TILE, TILE), 0).astype(jnp.float32)

    def step(k, carry):
        packed = list_ref[k]
        index = packed // 256
        col = (packed // 2) % 128
        flip = (packed % 2).astype(jnp.float32)
        sign = 1.0 - 2.0 * flip
        start = 128.0 * flip
        place = pos_ref[index]
        value = res_ref[index]
        row_taps = taps(row_cells * sign + start, place[0:1, :])
        col_taps = taps(col_cells * sign + start, place[1:2, :])
        weighted = jnp.concatenate(
            [col_taps * value[0:1, :], col_taps * (value[1:2, :] * sign)], axis=0
        )
        rh, rm, rl = split_three(row_taps)
        wh, wm, wl = split_three(weighted)
        left = jnp.concatenate([rh, rh, rh, rm, rm, rl], axis=1)
        right = jnp.concatenate([wh, wm, wl, wh, wm, wh], axis=1)
        sub = lax.dot_general(
            left, right, (((1,), (1,)), ((), ())), preferred_element_type=jnp.float32
        )
        out_ref[0, col] += sub[:, :TILE]
        out_ref[1, col] += sub[:, TILE:]
        return carry

    lax.fori_loop(0, count, step, 0)


def grid_rows(info, table, residual, position, rows):
    tiles = G // TILE
    smem = pl.BlockSpec(memory_space=pltpu.SMEM)
    vmem = pl.BlockSpec(memory_space=pltpu.VMEM)
    return pl.pallas_call(
        functools.partial(grid_kernel, rows),
        out_shape=jax.ShapeDtypeStruct((2, tiles, rows, TILE), jnp.float32),
        in_specs=[smem, smem, vmem, vmem],
        out_specs=vmem,
        compiler_params=pltpu.CompilerParams(vmem_limit_bytes=56 * 1024 * 1024),
        cost_estimate=pl.CostEstimate(
            flops=2 * 10**10, bytes_accessed=16 * 2**20, transcendentals=0
        ),
        name="grid_rows",
    )(info, table, residual, position)


def einsum(form, *args, precision=lax.Precision.HIGH):
    return jnp.einsum(form, *args, precision=precision, preferred_element_type=jnp.float32)


def per_device(residual, position, owner, tile_local, xi, amplitude):
    n = lax.axis_size(both)
    n_base = lax.axis_size("base")
    n_slab = lax.axis_size("slab")
    me = lax.axis_index(both)
    rows, size = xi.shape
    depth = size // n
    half = depth // 2
    tiles = G // TILE

    region_rows = G // n_slab // TILE
    region_cols = G // n_base // TILE
    target = owner[:, 0]
    tile_row = (target % n_slab) * region_rows + tile_local // region_cols
    tile_col = (target // n_slab) * region_cols + tile_local % region_cols
    flip = tile_row >= tiles // 2
    tile_row = jnp.where(flip, tiles - 1 - tile_row, tile_row)
    tile_col = jnp.where(flip, tiles - 1 - tile_col, tile_col)
    code = tile_row * 256 + tile_col * 2 + flip.astype(jnp.int32)
    codes = lax.all_gather(code, both, axis=0, tiled=True)
    all_res = lax.all_gather(residual, both, axis=0, tiled=True)
    all_pos = lax.all_gather(position, both, axis=0, tiled=True)
    blocks = codes.shape[0]
    grid_depth = G // 2 // n
    first_row = me * grid_depth
    mine = (codes // 256 == first_row // TILE).astype(jnp.int32)
    rank = jnp.where(mine == 1, jnp.cumsum(mine) - 1, -1)
    packed = lax.broadcasted_iota(jnp.int32, (blocks,), 0) * 256 + codes % 256
    spots = lax.broadcasted_iota(jnp.int32, (blocks, blocks), 0)
    table = jnp.sum(jnp.where(spots == rank[None, :], packed[None, :], 0), axis=1)
    info = jnp.stack([jnp.sum(mine), first_row % TILE]).astype(jnp.int32)

    outer, inner = row_tables(n, size)
    spectrum = (amplitude * xi).reshape(rows, n, depth)
    mid = einsum("rba,bqc->qcra", spectrum, outer)
    sent = einsum("cra,cae->cre", mid[0], inner[:, 0]) + einsum("cra,cae->cre", mid[1], inner[:, 1])
    field = lax.all_to_all(sent, both, split_axis=0, concat_axis=0, tiled=True)
    field = field.reshape(size, depth)
    lane = lax.broadcasted_iota(jnp.int32, (1, depth), 1)
    still = (me == 0) & (lane % half == 0)

    def mirror(x):
        return jnp.where(still, x, jnp.roll(x, half, axis=-1))

    c_len = 128
    d_len = size // c_len
    bc, bs = (x.astype(np.float32) for x in trig(np.arange(c_len)[:, None] * np.arange(c_len)[None, :], c_len))
    shape = (c_len, d_len, depth)
    n0 = c_len * np.arange(d_len)[None, :] + np.arange(c_len)[:, None]
    ic, isn = (x.astype(np.float32) for x in trig(n0[:, :, None] * np.arange(d_len)[None, None, :], size))
    pair = jnp.stack([field.reshape(shape), mirror(field).reshape(shape)])
    first = np.stack([np.stack([bc, bs], 1), np.stack([bs, -bc], 1)], 0)
    turned = einsum("qbal,qbsc->csal", pair, first)
    second = np.stack([ic, -isn], axis=2)
    power = einsum("csal,cdsa->cdl", turned, second)
    sky = jnp.exp(power / size)

    grid = grid_rows(info, table, all_res, all_pos, grid_depth)
    outer_g, low_g, high_g = grid_row_tables(n, size)
    parts = tiles // n if tiles >= n else 1
    inner_len = G // n
    if inner_len >= TILE:
        view = grid.reshape(2, n, inner_len // TILE, grid_depth, TILE)
    else:
        flat = grid.transpose(0, 2, 1, 3).reshape(2, grid_depth, n, inner_len)
        view = flat.transpose(0, 2, 1, 3)[:, :, None]
        parts = 1
    lanes = view.shape[-1]
    stage = einsum("qbpra,qbsc->cspra", view, outer_g, precision=fine)
    tab = (n, 2, parts, lanes, depth)
    low = einsum("cspra,cspae->cre", stage, low_g.reshape(tab), precision=fine)
    high = einsum("cspra,cspae->cre", stage, high_g.reshape(tab), precision=fine)
    high = jnp.concatenate([high[:1], jnp.flip(high[1:], axis=0)], axis=0)
    low = lax.all_to_all(low, both, split_axis=0, concat_axis=0, tiled=True).reshape(size, depth)
    high = lax.all_to_all(high, both, split_axis=0, concat_axis=0, tiled=True).reshape(size, depth)
    real = jnp.concatenate([low[:, :half], high[:, :half]], axis=1)
    imag = jnp.concatenate([low[:, half:], high[:, half:]], axis=1)
    wide = G // c_len
    deep = size // wide
    gc, gs = (x.astype(np.float32) for x in trig(np.arange(deep)[:, None] * np.arange(c_len)[None, :], c_len))
    first_g = np.stack([np.stack([gc, gs], 1), np.stack([-gs, gc], 1)], 0)
    whole = jnp.stack([real.reshape(deep, wide, depth), imag.reshape(deep, wide, depth)])
    turned_g = einsum("qbal,qbsc->csal", whole, first_g, precision=fine)
    ac, asn = trig((n0 + G // 4)[:, :, None] * np.arange(wide)[None, None, :], G)
    second_g = (np.stack([ac, -asn], axis=2) / G).astype(np.float32)
    back = einsum("csal,cdsa->cdl", turned_g, second_g, precision=fine)

    z = sky * back
    pz = einsum("cdl,cda->cal", z, ic)
    qz = einsum("cdl,cda->cal", z, isn)
    joined = jnp.stack([pz + mirror(qz), mirror(pz) - qz])
    fold = einsum("qcal,qcb->bal", joined, np.stack([bc, bs]))
    folded = lax.all_to_all(
        fold.reshape(n, rows, depth), both, split_axis=0, concat_axis=0, tiled=True
    )
    ends = einsum("jre,jqae->qjra", folded, inner)
    final = einsum("qjra,bqj->rba", ends, outer)
    return amplitude * final.reshape(rows, size) / size


def solution(mesh):
    placed = (
        P(both, None, None),
        P(both, None, None),
        P(both, None),
        P(both),
        P(both, None),
        P(both, None),
    )
    return jax.shard_map(
        per_device, mesh=mesh, in_specs=placed, out_specs=P(both, None), check_vma=False
    )
```

```python
import functools

import jax
import jax.numpy as jnp
import numpy as np
from jax import lax
from jax.experimental import pallas as pl
from jax.experimental.pallas import tpu as pltpu
from jax.sharding import PartitionSpec as P

G = 8192
TILE = 128
both = ("base", "slab")
fine = lax.Precision.HIGHEST


def trig(product, modulus):
    angle = (product % modulus).astype(np.float64) * (2.0 * np.pi / modulus)
    return np.cos(angle), np.sin(angle)


def column_table(n, size):
    depth = size // n
    half = depth // 2
    i = np.arange(half)[None, :]
    j = np.arange(n)[:, None]
    low = n * i + j
    high = (-low) % size
    high[0, 0] = size // 2
    return np.concatenate([low, high], axis=1)


def row_tables(n, size):
    depth = size // n
    cols = column_table(n, size)
    oc, osn = trig(np.arange(n)[:, None] * np.arange(n)[None, :], n)
    outer = np.stack([oc, osn], axis=1)
    prod = np.arange(depth)[None, :, None] * cols[:, None, :]
    c, s = trig(prod, size)
    sign = np.where(np.arange(depth) < depth // 2, 1.0, -1.0)[None, None, :]
    inner = np.stack([c + s, sign * (c - s)], axis=1)
    return outer.astype(np.float32), inner.astype(np.float32)


def grid_row_tables(n, size):
    depth = G // n
    cols = column_table(n, size)
    half = cols.shape[1] // 2
    oc, osn = trig(np.arange(n)[:, None] * np.arange(n)[None, :], n)
    outer = np.stack([np.stack([oc, osn], 1), np.stack([-osn, oc], 1)], 0)
    low = cols[:, :half]
    high = cols[(-np.arange(n)) % n, half:]
    a = np.arange(depth)[None, :, None]
    out = []
    for part in (low, high):
        c, s = trig(a * (part[:, None, :] + G // 4), G)
        out.append(np.stack([np.concatenate([c, s], 2), np.concatenate([-s, c], 2)], 1))
    return outer.astype(np.float32), np.concatenate(out, axis=3).astype(np.float32)


def taps(cells, offsets):
    scaled = (cells - offsets) * 0.25
    kept = jnp.maximum(1.0 - scaled * scaled, 0.0)
    return kept * kept * kept


def split_three(x):
    high = x.astype(jnp.bfloat16)
    rest = x - high.astype(jnp.float32)
    middle = rest.astype(jnp.bfloat16)
    return high, middle, (rest - middle.astype(jnp.float32)).astype(jnp.bfloat16)


def grid_kernel(rows, info_ref, list_ref, data_ref, out_ref):
    count = info_ref[0]
    first = info_ref[1].astype(jnp.float32)
    out_ref[...] = jnp.zeros_like(out_ref)
    row_cells = lax.broadcasted_iota(jnp.int32, (rows, TILE), 0).astype(jnp.float32) + first
    col_cells = lax.broadcasted_iota(jnp.int32, (TILE, TILE), 0).astype(jnp.float32)

    def step(k, carry):
        packed = list_ref[k]
        index = packed // 256
        col = (packed // 2) % 128
        flip = (packed % 2).astype(jnp.float32)
        sign = 1.0 - 2.0 * flip
        start = 128.0 * flip
        block = data_ref[index]
        value = block[0:2, :]
        place = block[2:4, :]
        row_taps = taps(row_cells * sign + start, place[0:1, :])
        col_taps = taps(col_cells * sign + start, place[1:2, :])
        weighted = jnp.concatenate(
            [col_taps * value[0:1, :], col_taps * (value[1:2, :] * sign)], axis=0
        )
        rh, rm, rl = split_three(row_taps)
        wh, wm, wl = split_three(weighted)
        left = jnp.concatenate([rh, rh, rh, rm, rm, rl], axis=1)
        right = jnp.concatenate([wh, wm, wl, wh, wm, wh], axis=1)
        sub = lax.dot_general(
            left, right, (((1,), (1,)), ((), ())), preferred_element_type=jnp.float32
        )
        out_ref[0, col] += sub[:, :TILE]
        out_ref[1, col] += sub[:, TILE:]
        return carry

    lax.fori_loop(0, count, step, 0)


def grid_rows(info, table, gathered, rows):
    tiles = G // TILE
    smem = pl.BlockSpec(memory_space=pltpu.SMEM)
    vmem = pl.BlockSpec(memory_space=pltpu.VMEM)
    return pl.pallas_call(
        functools.partial(grid_kernel, rows),
        out_shape=jax.ShapeDtypeStruct((2, tiles, rows, TILE), jnp.float32),
        in_specs=[smem, smem, vmem],
        out_specs=vmem,
        compiler_params=pltpu.CompilerParams(vmem_limit_bytes=56 * 1024 * 1024),
        cost_estimate=pl.CostEstimate(
            flops=2 * 10**10, bytes_accessed=16 * 2**20, transcendentals=0
        ),
        name="grid_rows",
    )(info, table, gathered)


def einsum(form, *args, precision=lax.Precision.HIGH):
    return jnp.einsum(form, *args, precision=precision, preferred_element_type=jnp.float32)


def per_device(residual, position, owner, tile_local, xi, amplitude):
    n = lax.axis_size(both)
    n_base = lax.axis_size("base")
    n_slab = lax.axis_size("slab")
    me = lax.axis_index(both)
    rows, size = xi.shape
    depth = size // n
    half = depth // 2
    tiles = G // TILE

    region_rows = G // n_slab // TILE
    region_cols = G // n_base // TILE
    target = owner[:, 0]
    tile_row = (target % n_slab) * region_rows + tile_local // region_cols
    tile_col = (target // n_slab) * region_cols + tile_local % region_cols
    flip = tile_row >= tiles // 2
    tile_row = jnp.where(flip, tiles - 1 - tile_row, tile_row)
    tile_col = jnp.where(flip, tiles - 1 - tile_col, tile_col)
    code = tile_row * 256 + tile_col * 2 + flip.astype(jnp.int32)
    codes = lax.all_gather(code, both, axis=0, tiled=True)
    payload = jnp.concatenate([residual, position], axis=1)
    codes, payload = lax.optimization_barrier((codes, payload))
    gathered = lax.all_gather(payload, both, axis=0, tiled=True)
    blocks = codes.shape[0]
    grid_depth = G // 2 // n
    first_row = me * grid_depth
    mine = (codes // 256 == first_row // TILE).astype(jnp.int32)
    rank = jnp.where(mine == 1, jnp.cumsum(mine) - 1, -1)
    packed = lax.broadcasted_iota(jnp.int32, (blocks,), 0) * 256 + codes % 256
    spots = lax.broadcasted_iota(jnp.int32, (blocks, blocks), 0)
    table = jnp.sum(jnp.where(spots == rank[None, :], packed[None, :], 0), axis=1)
    info = jnp.stack([jnp.sum(mine), first_row % TILE]).astype(jnp.int32)

    outer, inner = row_tables(n, size)
    spectrum = (amplitude * xi).reshape(rows, n, depth)
    mid = einsum("rba,bqc->qcra", spectrum, outer)
    sent = einsum("cra,cae->cre", mid[0], inner[:, 0]) + einsum("cra,cae->cre", mid[1], inner[:, 1])
    sent, gathered = lax.optimization_barrier((sent, gathered))
    field = lax.all_to_all(sent, both, split_axis=0, concat_axis=0, tiled=True)
    field = field.reshape(size, depth)
    lane = lax.broadcasted_iota(jnp.int32, (1, depth), 1)
    still = (me == 0) & (lane % half == 0)

    def mirror(x):
        return jnp.where(still, x, jnp.roll(x, half, axis=-1))

    c_len = 128
    d_len = size // c_len
    bc, bs = (x.astype(np.float32) for x in trig(np.arange(c_len)[:, None] * np.arange(c_len)[None, :], c_len))
    shape = (c_len, d_len, depth)
    n0 = c_len * np.arange(d_len)[None, :] + np.arange(c_len)[:, None]
    ic, isn = (x.astype(np.float32) for x in trig(n0[:, :, None] * np.arange(d_len)[None, None, :], size))
    pair = jnp.stack([field.reshape(shape), mirror(field).reshape(shape)])
    first = np.stack([np.stack([bc, bs], 1), np.stack([bs, -bc], 1)], 0)
    turned = einsum("qbal,qbsc->csal", pair, first)
    second = np.stack([ic, -isn], axis=2)
    power = einsum("csal,cdsa->cdl", turned, second)
    sky = jnp.exp(power / size)

    grid = grid_rows(info, table, gathered, grid_depth)
    outer_g, inner_g = grid_row_tables(n, size)
    parts = tiles // n if tiles >= n else 1
    inner_len = G // n
    if inner_len >= TILE:
        view = grid.reshape(2, n, inner_len // TILE, grid_depth, TILE)
    else:
        flat = grid.transpose(0, 2, 1, 3).reshape(2, grid_depth, n, inner_len)
        view = flat.transpose(0, 2, 1, 3)[:, :, None]
        parts = 1
    lanes = view.shape[-1]
    stage = einsum("qbpra,qbsc->cspra", view, outer_g, precision=fine)
    inner_g = inner_g.reshape(n, 2, parts, lanes, 2 * depth)
    halves = einsum("cspra,cspae->cre", stage, inner_g, precision=fine)
    high = halves[:, :, depth:]
    high = jnp.concatenate([high[:1], jnp.flip(high[1:], axis=0)], axis=0)
    halves = jnp.concatenate([halves[:, :, :depth], high], axis=2)
    got = lax.all_to_all(halves, both, split_axis=0, concat_axis=0, tiled=True)
    got = got.reshape(size, 2 * depth)
    real = jnp.concatenate([got[:, :half], got[:, depth : depth + half]], axis=1)
    imag = jnp.concatenate([got[:, half:depth], got[:, depth + half :]], axis=1)
    wide = G // c_len
    deep = size // wide
    gc, gs = (x.astype(np.float32) for x in trig(np.arange(deep)[:, None] * np.arange(c_len)[None, :], c_len))
    first_g = np.stack([np.stack([gc, gs], 1), np.stack([-gs, gc], 1)], 0)
    whole = jnp.stack([real.reshape(deep, wide, depth), imag.reshape(deep, wide, depth)])
    turned_g = einsum("qbal,qbsc->csal", whole, first_g, precision=fine)
    ac, asn = trig((n0 + G // 4)[:, :, None] * np.arange(wide)[None, None, :], G)
    second_g = (np.stack([ac, -asn], axis=2) / G).astype(np.float32)
    back = einsum("csal,cdsa->cdl", turned_g, second_g, precision=fine)

    z = sky * back
    pz = einsum("cdl,cda->cal", z, ic)
    qz = einsum("cdl,cda->cal", z, isn)
    joined = jnp.stack([pz + mirror(qz), mirror(pz) - qz])
    fold = einsum("qcal,qcb->bal", joined, np.stack([bc, bs]))
    folded = lax.all_to_all(
        fold.reshape(n, rows, depth), both, split_axis=0, concat_axis=0, tiled=True
    )
    ends = einsum("jre,jqae->qjra", folded, inner)
    final = einsum("qjra,bqj->rba", ends, outer)
    return amplitude * final.reshape(rows, size) / size


def solution(mesh):
    placed = (
        P(both, None, None),
        P(both, None, None),
        P(both, None),
        P(both),
        P(both, None),
        P(both, None),
    )
    return jax.shard_map(
        per_device, mesh=mesh, in_specs=placed, out_specs=P(both, None), check_vma=False
    )
```
